128 devices in a mesh: blk: 64 (over x, y_lo, z, core), grp: 2 (over y_hi).
Axes of the slice: x: 4, y: 4 (y_hi: 2, y_lo: 2; y = y_hi * 2 + y_lo), z: 4, core: 2. Of those that a mesh axis runs over, the one named last changes fastest.
Arguments:
- left_real: bfloat16 [16384, 8192], P('blk'), may hold values from -6 to 6
- left_imag: bfloat16 [16384, 8192], P('blk'), may hold values from -6 to 6
- right_real: bfloat16 [8192, 512], P('blk', 'grp'), may hold values from -0.0625 to 0.0625
- right_imag: bfloat16 [8192, 512], P('blk', 'grp'), may hold values from -0.0625 to 0.0625
- row_scale: float32 [16384], P('blk'), may hold values from 0.25 to 4
- bond_order: int32 [8192], replicated, may hold values from 0 to 8191, each once
Outputs:
- result_real: float32 [16384, 512], P('blk', 'grp')
- result_imag: float32 [16384, 512], P('blk', 'grp')
The draws below stay inside these ranges and needn't reach their ends.
Inputs may be any that keep to these rules, and one draw needn't show every extreme that they name: bond_order names each of 0 to 8191 exactly once.
All inputs are finite; a program needn't handle non-finite values.
Results may differ from the reference program's by a relative error of at most 0.0003.
Values may be sent and summed in bfloat16 or wider, within the bound.
A program may use at most 128 MiB of HBM per device.

```python
import math
import jax
import jax.numpy as jnp
from jax import lax

BOND = 8192
COLS = 512
ROWS = 16384


def levels(stream_key, extent, pieces, low, high):
    factor_of = 1.0
    for axis_at, blocks in pieces:
        heights = jax.random.uniform(jax.random.fold_in(jax.random.fold_in(stream_key, 6), axis_at), (blocks,), jnp.float32, low / len(pieces), high / len(pieces))
        factor_of = factor_of * jnp.repeat(jnp.exp(heights), extent[axis_at] // blocks).reshape((-1,) + (1,) * (len(extent) - 1 - axis_at))
    return factor_of


def normal_values(rng, shape, width, most, pieces=(), kind=jnp.bfloat16):
    drawn = width * jax.random.normal(rng, shape, jnp.float32)
    if pieces:
        drawn = drawn * levels(rng, shape, pieces, -0.22, 0.18)
    return jnp.clip(drawn, -most, most).astype(kind)


def setup_inputs(seed: int = 0) -> dict:
    splits = jax.random.split(jax.random.key(seed), 7)
    return {
        "left_real": normal_values(splits[0], (ROWS, BOND), 1.0, 6.0, ((0, 64),)),
        "left_imag": normal_values(splits[1], (ROWS, BOND), 1.0, 6.0, ((0, 64),)),
        "right_real": normal_values(splits[2], (BOND, COLS), BOND ** -0.5, 0.0625, ((0, 64), (1, 2))),
        "right_imag": normal_values(splits[3], (BOND, COLS), BOND ** -0.5, 0.0625, ((0, 64), (1, 2))),
        "row_scale": jnp.clip(jnp.exp(math.log(4.0) - 2.7725887 * jax.random.uniform(splits[4], (ROWS,), jnp.float32) ** levels(splits[4], (ROWS,), ((0, 64),), -0.2, 0.2)), 0.25, 4.0),
        "bond_order": jax.random.permutation(splits[5], BOND).astype(jnp.int32),
    }


def product(left, right):
    return jnp.dot(left.astype(jnp.float32), right.astype(jnp.float32), precision=lax.Precision.HIGHEST)

def reference(left_real, left_imag, right_real, right_imag, row_scale, bond_order):
    order = bond_order.astype(jnp.int32)
    perm_real = jnp.take(left_real, order, axis=1)
    perm_imag = jnp.take(left_imag, order, axis=1)
    raw_real = product(perm_real, right_real) - product(perm_imag, right_imag)
    raw_imag = product(perm_real, right_imag) + product(perm_imag, right_real)
    scaled_real = raw_real * row_scale[:, None]
    scaled_imag = raw_imag * row_scale[:, None]
    total = jnp.sum(scaled_real * scaled_real + scaled_imag * scaled_imag)
    factor = 1.0 / jnp.sqrt(total / jnp.float32(ROWS * COLS))
    return (scaled_real * factor, scaled_imag * factor)
```

```python
import functools
import heapq

import jax
import jax.numpy as jnp
from jax import lax
from jax.experimental import pallas as pl
from jax.experimental.pallas import tpu as pltpu
from jax.sharding import PartitionSpec as P

MESH = pl.DeviceIdType.MESH
LANES = 128
HALF = 2
STAGES = 8
UNROLL = 16
TILES = 8
NX, NY, NZ = 4, 2, 4
DO_COMM, DO_TURN, DO_PICK, DO_MM = True, True, True, True
HOP_US, WIRE_US = 2.4, 0.7
START_US = 2.0
SLACK_US = 0.2
TURN_US, PICK_US = 0.08, 0.3

XP, XM, ZP, ZM, YY = range(5)


def plan():
    events = []
    free = [0.0] * 5
    queue = []
    count = 0

    def send(now, link, half, travel, pieces):
        nonlocal count
        start = max(now, free[link])
        free[link] = start + WIRE_US * len(pieces)
        count += 1
        heapq.heappush(queue, (free[link] + HOP_US, count, link, half, travel, pieces))

    def moved(travel, link):
        dx, dy, dz = travel
        return {
            XP: (dx + 1, dy, dz), XM: (dx - 1, dy, dz), YY: (dx, 1, dz),
            ZP: (dx, dy, dz + 1), ZM: (dx, dy, dz - 1),
        }[link]

    rings = {0: ((XP, XM), (ZP, ZM)), 1: ((ZP, ZM), (XP, XM))}

    def onward(link, half, travel, pieces):
        first, second = rings[half]
        out = []
        stage = 0 if link in first else 1 if link == YY else 2 if link in second else -1
        ring = first if stage == 0 else second if stage == 2 else None
        if ring is not None:
            hops = abs(travel[0] if ring[0] == XP else travel[2])
            if hops == 1:
                mine = tuple(p for p in pieces if p == ring.index(link))
                if mine:
                    out.append((link, mine))
        if stage == -1:
            out += [(k, pieces) for k in first]
        if stage <= 0:
            out.append((YY, pieces))
        if stage <= 1:
            out += [(k, pieces) for k in second]
        return out

    own = [[], []]
    for half in (0, 1):
        own[half] = onward(None, half, (0, 0, 0), (0, 1))
    starts = []
    for pair in zip(*own):
        for half, (link, pieces) in enumerate(pair):
            starts.append((half, link, pieces))
    for half, link, pieces in starts:
        send(0.0, link, half, moved((0, 0, 0), link), pieces)
    while queue:
        now, _, link, half, travel, pieces = heapq.heappop(queue)
        follow = onward(link, half, travel, pieces)
        events.append((now, link, half, travel, pieces, follow))
        for k, p in follow:
            send(now, k, half, moved(travel, k), p)
    return starts, events, moved


def kernel(
    devices,
    lr_hbm, li_hbm, rr_ref, ri_ref, scale_ref, order_ref,
    out_r, out_i, total_ref,
    left_v, table, picked, perm, held, acc,
    left_sem, ring_send, ring_recv, pair_send, pair_recv,
    sums, sum_send, sum_recv,
):
    rows, bond = lr_hbm.shape
    depth, cols = rr_ref.shape
    chips = devices // 2
    per = rows // LANES
    words = 2 * per
    width = bond // STAGES
    piece = 2 * cols // (2 * HALF)

    me = lax.axis_index("blk")
    chip, core = me // 2, lax.rem(me, 2)
    other = 1 - core
    z = lax.rem(chip, NZ)
    y = lax.rem(chip // NZ, NY)
    x = chip // (NZ * NY)
    wrap_x = [lax.rem(x + NX - d, NX) for d in range(NX)]
    wrap_z = [lax.rem(z + NZ - d, NZ) for d in range(NZ)]
    flip_y = [y, 1 - y]

    def chip_of(travel):
        dx, dy, dz = travel
        return (wrap_x[dx % NX] * NY + flip_y[dy]) * NZ + wrap_z[dz % NZ]

    ahead = {
        XP: chip_of((-1, 0, 0)) * 2 + core, XM: chip_of((1, 0, 0)) * 2 + core,
        ZP: chip_of((0, 0, -1)) * 2 + core, ZM: chip_of((0, 0, 1)) * 2 + core,
        YY: chip_of((0, 1, 0)) * 2 + core,
    }
    partner = chip * 2 + other

    def read_left(stage):
        return [
            pltpu.make_async_copy(
                src.at[:, pl.ds(stage * width, width)],
                left_v.at[n, stage],
                left_sem.at[n, stage],
            )
            for n, src in enumerate((lr_hbm, li_hbm))
        ]

    for stage in range(STAGES):
        for copy in read_left(stage):
            copy.start()

    barrier = pltpu.get_barrier_semaphore()
    for o in range(1, devices):
        target = lax.rem(me + o, devices)
        pl.semaphore_signal(barrier, inc=1, device_id={"blk": target}, device_id_type=MESH)

    for n, ref in enumerate((rr_ref, ri_ref)):
        held[me, n * cols:(n + 1) * cols, :] = (
            ref[...].astype(jnp.float32).T.astype(jnp.bfloat16)
        )
    acc[...] = jnp.zeros_like(acc)
    pl.semaphore_wait(barrier, devices - 1)

    starts, events, moved = plan()
    slots = {}
    for i, (_, link, half, travel, pieces, _) in enumerate(events):
        slots[(link, half, travel, pieces)] = i

    def part(where, which, half, pieces):
        first = (half * HALF + pieces[0]) * piece
        return held.at[where * 2 + which, pl.ds(first, piece * len(pieces)), :]

    def ring_copy(link, half, travel, pieces, after):
        ref = part(chip_of(travel), core, half, pieces)
        return pltpu.make_async_remote_copy(
            src_ref=ref, dst_ref=ref,
            send_sem=ring_send.at[slots[(link, half, after, pieces)]],
            recv_sem=ring_recv.at[slots[(link, half, after, pieces)]],
            device_id={"blk": ahead[link]}, device_id_type=MESH,
        )

    def pair_copy(event, which):
        if event is None:
            ref, slot = held.at[chip * 2 + which], len(events)
        else:
            _, link, half, travel, pieces, _ = event
            ref = part(chip_of(travel), which, half, pieces)
            slot = slots[(link, half, travel, pieces)]
        return pltpu.make_async_remote_copy(
            src_ref=ref, dst_ref=ref,
            send_sem=pair_send.at[slot], recv_sem=pair_recv.at[slot],
            device_id={"blk": partner}, device_id_type=MESH,
        )

    def begin():
        if not DO_COMM:
            return
        here = (0, 0, 0)
        for half, link, pieces in starts:
            ring_copy(link, half, here, pieces, moved(here, link)).start()
        pair_copy(None, core).start()

    def arrive(event):
        if not DO_COMM:
            return
        _, link, half, travel, pieces, follow = event
        ring_copy(link, half, travel, pieces, travel).wait_recv()
        for k, p in follow:
            ring_copy(k, half, travel, p, moved(travel, k)).start()
        pair_copy(event, core).start()

    def turn(stage):
        for copy in read_left(stage):
            copy.wait()

    def turn_tiles(stage, first, last):
        if not DO_TURN:
            return

        def step(t, _):
            at = pl.multiple_of(t * LANES, LANES)
            for n in range(2):
                for h in range(per):
                    tile = left_v[n, stage, h * LANES:(h + 1) * LANES, pl.ds(at, LANES)]
                    row = pl.multiple_of(stage * width + at, LANES)
                    table[pl.ds(row, LANES), n * per + h, :] = tile.astype(jnp.float32).T
            return 0

        lax.fori_loop(first, last, step, 0, unroll=2)

    def pick(block):
        if not DO_PICK:
            return
        base = block * depth

        def step(s, _):
            at = s * UNROLL
            got = []
            for u in range(UNROLL):
                got.append(table[order_ref[base + at + u]])
            for u in range(UNROLL):
                picked[pl.ds(pl.multiple_of((at + u) * words, words), words), :] = got[u]
            return 0

        lax.fori_loop(0, depth // UNROLL, step, 0)
        for w in range(words):
            perm[block, :, w * LANES:(w + 1) * LANES] = picked[
                pl.ds(w, depth, stride=words), :
            ].astype(jnp.bfloat16)

    def pick_some(first, last):
        lax.fori_loop(first, last, lambda b, _: (pick(b), 0)[1], 0)

    work = []
    for stage in range(STAGES):
        work.append((0.0, functools.partial(turn, stage)))
        for t in range(0, width // LANES, TILES):
            work.append((TILES * TURN_US, functools.partial(turn_tiles, stage, t, t + TILES)))
    for b in range(0, devices, 8):
        work.append((8 * PICK_US, functools.partial(pick_some, b, b + 8)))

    begin()
    now = 0.0
    todo = list(events)
    for cost, item in work:
        while todo and todo[0][0] + SLACK_US <= now:
            arrive(todo.pop(0))
        item()
        now += cost
    for event in todo:
        arrive(event)
    if DO_COMM:
        for event in [None, *events]:
            pair_copy(event, other).wait_recv()

    def multiply(b, _):
        acc[...] += jnp.dot(held[b], perm[b], preferred_element_type=jnp.float32)
        return 0

    if DO_MM:
        lax.fori_loop(0, devices, multiply, 0)

    low, high = pl.ds(0, cols), pl.ds(cols, cols)
    scale = scale_ref[...]
    real = (acc[low, 0:rows] - acc[high, rows:2 * rows]) * scale
    imag = (acc[low, rows:2 * rows] + acc[high, 0:rows]) * scale
    squares = jnp.sum(real * real + imag * imag, axis=0, keepdims=True)
    sums[me] = sum(squares[:, h * LANES:(h + 1) * LANES] for h in range(per))
    out_r[...] = real.T

    def sum_copy(o):
        return pltpu.make_async_remote_copy(
            src_ref=sums.at[me], dst_ref=sums.at[me],
            send_sem=sum_send.at[o - 1], recv_sem=sum_recv.at[o - 1],
            device_id={"blk": lax.rem(me + o, devices)}, device_id_type=MESH,
        )

    if DO_COMM:
        for o in range(1, devices):
            sum_copy(o).start()
    out_i[...] = imag.T
    if DO_COMM:
        def sum_wait(o):
            block = lax.rem(me + devices - o, devices)
            pltpu.make_async_remote_copy(
                src_ref=sums.at[block], dst_ref=sums.at[block],
                send_sem=sum_send.at[o - 1], recv_sem=sum_recv.at[o - 1],
                device_id={"blk": block}, device_id_type=MESH,
            ).wait()

        for o in range(1, devices):
            sum_wait(o)
    total_ref[...] = jnp.sum(jnp.sum(sums[...], axis=0), axis=1, keepdims=True)
    if DO_COMM:
        here = (0, 0, 0)
        for half, link, pieces in starts:
            ring_copy(link, half, here, pieces, moved(here, link)).wait_send()
        for _, _, half, travel, _, follow in events:
            for k, p in follow:
                ring_copy(k, half, travel, p, moved(travel, k)).wait_send()
        for event in [None, *events]:
            pair_copy(event, core).wait_send()


def body(devices, groups, left_real, left_imag, right_real, right_imag, row_scale, bond_order):
    rows, bond = left_real.shape
    depth, cols = right_real.shape
    messages = len(plan()[1])
    vmem = pl.BlockSpec(memory_space=pltpu.VMEM)
    far = pl.BlockSpec(memory_space=pl.ANY)
    words = 2 * rows // LANES
    out = jax.ShapeDtypeStruct((rows, cols), jnp.float32)
    real, imag, total = pl.pallas_call(
        functools.partial(kernel, devices),
        out_shape=(out, out, jax.ShapeDtypeStruct((1, 1), jnp.float32)),
        in_specs=[far, far, vmem, vmem, vmem, pl.BlockSpec(memory_space=pltpu.SMEM)],
        out_specs=(vmem, vmem, vmem),
        scratch_shapes=[
            pltpu.VMEM((2, STAGES, rows, bond // STAGES), jnp.bfloat16),
            pltpu.VMEM((bond, words, LANES), jnp.float32),
            pltpu.VMEM((depth * words, LANES), jnp.float32),
            pltpu.VMEM((devices, depth, 2 * rows), jnp.bfloat16),
            pltpu.VMEM((devices, 2 * cols, depth), jnp.bfloat16),
            pltpu.VMEM((2 * cols, 2 * rows), jnp.float32),
            pltpu.SemaphoreType.DMA((2, STAGES)),
            pltpu.SemaphoreType.DMA((messages,)),
            pltpu.SemaphoreType.DMA((messages,)),
            pltpu.SemaphoreType.DMA((messages + 1,)),
            pltpu.SemaphoreType.DMA((messages + 1,)),
            pltpu.VMEM((devices, 1, LANES), jnp.float32),
            pltpu.SemaphoreType.DMA((devices - 1,)),
            pltpu.SemaphoreType.DMA((devices - 1,)),
        ],
        compiler_params=pltpu.CompilerParams(
            collective_id=0, has_side_effects=True, vmem_limit_bytes=60 * 1024 * 1024
        ),
    )(left_real, left_imag, right_real, right_imag, row_scale.reshape(1, rows), bond_order)
    whole = total
    for o in range(1, groups):
        ring = [(g, (g + o) % groups) for g in range(groups)]
        whole = whole + lax.ppermute(total, "grp", ring)
    factor = 1.0 / jnp.sqrt(whole / jnp.float32(rows * cols * devices * groups))
    return real * factor, imag * factor


def solution(mesh):
    in_specs = (P("blk", None), P("blk", None), P("blk", "grp"), P("blk", "grp"), P("blk"), P())
    out_specs = (P("blk", "grp"), P("blk", "grp"))
    return jax.shard_map(
        functools.partial(body, mesh.shape["blk"], mesh.shape["grp"]),
        mesh=mesh, in_specs=in_specs, out_specs=out_specs, check_vma=False,
    )
```

```python
import functools
import heapq

import jax
import jax.numpy as jnp
from jax import lax
from jax.experimental import pallas as pl
from jax.experimental.pallas import tpu as pltpu
from jax.sharding import PartitionSpec as P

MESH = pl.DeviceIdType.MESH
LANES = 128
HALF = 2
STAGES = 8
UNROLL = 16
TILES = 8
RUN = 8
NX, NY, NZ = 4, 2, 4
DO_COMM, DO_TURN, DO_PICK, DO_MM = True, True, True, True
HOP_US, WIRE_US = 2.4, 0.7
START_US = 2.0
SLACK_US = 0.2
TURN_US, PICK_US = 0.18, 0.18
MULTIPLY_US, PAIR_US = 0.7, 1.2

XP, XM, ZP, ZM, YY = range(5)


def plan():
    events = []
    free = [0.0] * 5
    queue = []
    count = 0

    def send(now, link, half, travel, pieces):
        nonlocal count
        start = max(now, free[link])
        free[link] = start + WIRE_US * len(pieces)
        count += 1
        heapq.heappush(queue, (free[link] + HOP_US, count, link, half, travel, pieces))

    def moved(travel, link):
        dx, dy, dz = travel
        return {
            XP: (dx + 1, dy, dz), XM: (dx - 1, dy, dz), YY: (dx, 1, dz),
            ZP: (dx, dy, dz + 1), ZM: (dx, dy, dz - 1),
        }[link]

    rings = {0: ((XP, XM), (ZP, ZM)), 1: ((ZP, ZM), (XP, XM))}

    def onward(link, half, travel, pieces):
        first, second = rings[half]
        out = []
        stage = 0 if link in first else 1 if link == YY else 2 if link in second else -1
        ring = first if stage == 0 else second if stage == 2 else None
        if ring is not None:
            hops = abs(travel[0] if ring[0] == XP else travel[2])
            if hops == 1:
                mine = tuple(p for p in pieces if p == ring.index(link))
                if mine:
                    out.append((link, mine))
        if stage == -1:
            out += [(k, pieces) for k in first]
        if stage <= 0:
            out.append((YY, pieces))
        if stage <= 1:
            out += [(k, pieces) for k in second]
        return out

    own = [[], []]
    for half in (0, 1):
        own[half] = onward(None, half, (0, 0, 0), (0, 1))
    starts = []
    for pair in zip(*own):
        for half, (link, pieces) in enumerate(pair):
            starts.append((half, link, pieces))
    for half, link, pieces in starts:
        send(0.0, link, half, moved((0, 0, 0), link), pieces)
    while queue:
        now, _, link, half, travel, pieces = heapq.heappop(queue)
        follow = onward(link, half, travel, pieces)
        events.append((now, link, half, travel, pieces, follow))
        for k, p in follow:
            send(now, k, half, moved(travel, k), p)
    return starts, events, moved


def kernel(
    devices,
    lr_hbm, li_hbm, rr_ref, ri_ref, scale_ref, order_ref,
    out_r, out_i, total_ref,
    left_v, table, picked, perm, held, acc,
    left_sem, ring_send, ring_recv, pair_send, pair_recv,
    sums, sum_send, sum_recv,
):
    rows, bond = lr_hbm.shape
    depth, cols = rr_ref.shape
    chips = devices // 2
    per = rows // LANES
    words = 2 * per
    width = bond // STAGES
    piece = 2 * cols // (2 * HALF)

    me = lax.axis_index("blk")
    chip, core = me // 2, lax.rem(me, 2)
    other = 1 - core
    z = lax.rem(chip, NZ)
    y = lax.rem(chip // NZ, NY)
    x = chip // (NZ * NY)
    wrap_x = [lax.rem(x + NX - d, NX) for d in range(NX)]
    wrap_z = [lax.rem(z + NZ - d, NZ) for d in range(NZ)]
    flip_y = [y, 1 - y]

    def chip_of(travel):
        dx, dy, dz = travel
        return (wrap_x[dx % NX] * NY + flip_y[dy]) * NZ + wrap_z[dz % NZ]

    ahead = {
        XP: chip_of((-1, 0, 0)) * 2 + core, XM: chip_of((1, 0, 0)) * 2 + core,
        ZP: chip_of((0, 0, -1)) * 2 + core, ZM: chip_of((0, 0, 1)) * 2 + core,
        YY: chip_of((0, 1, 0)) * 2 + core,
    }
    partner = chip * 2 + other

    def read_left(stage):
        return [
            pltpu.make_async_copy(
                src.at[:, pl.ds(stage * width, width)],
                left_v.at[n, stage],
                left_sem.at[n, stage],
            )
            for n, src in enumerate((lr_hbm, li_hbm))
        ]

    for stage in range(STAGES):
        for copy in read_left(stage):
            copy.start()

    barrier = pltpu.get_barrier_semaphore()
    for o in range(1, devices):
        target = lax.rem(me + o, devices)
        pl.semaphore_signal(barrier, inc=1, device_id={"blk": target}, device_id_type=MESH)

    for n, ref in enumerate((rr_ref, ri_ref)):
        held[me, n * cols:(n + 1) * cols, :] = (
            ref[...].astype(jnp.float32).T.astype(jnp.bfloat16)
        )
    acc[...] = jnp.zeros_like(acc)
    pl.semaphore_wait(barrier, devices - 1)

    starts, events, moved = plan()
    slots = {}
    for i, (_, link, half, travel, pieces, _) in enumerate(events):
        slots[(link, half, travel, pieces)] = i

    def part(where, which, half, pieces):
        first = (half * HALF + pieces[0]) * piece
        return held.at[where * 2 + which, pl.ds(first, piece * len(pieces)), :]

    def ring_copy(link, half, travel, pieces, after):
        ref = part(chip_of(travel), core, half, pieces)
        return pltpu.make_async_remote_copy(
            src_ref=ref, dst_ref=ref,
            send_sem=ring_send,
            recv_sem=ring_recv.at[slots[(link, half, after, pieces)]],
            device_id={"blk": ahead[link]}, device_id_type=MESH,
        )

    batch = 4
    needs = {}
    for event in events:
        dx, dy, dz = event[3]
        needs.setdefault((dx % NX, dy, dz % NZ), []).append(event)
    near = sorted(needs, key=lambda k: max(e[0] for e in needs[k]))
    near = [(0, 0, 0), *near]
    turn_of = {t: i // batch for i, t in enumerate(near)}

    def pair_copy(ref, slot):
        return pltpu.make_async_remote_copy(
            src_ref=ref, dst_ref=ref, send_sem=pair_send, recv_sem=pair_recv.at[slot],
            device_id={"blk": partner}, device_id_type=MESH,
        )

    def begin():
        if not DO_COMM:
            return
        here = (0, 0, 0)
        for half, link, pieces in starts:
            ring_copy(link, half, here, pieces, moved(here, link)).start()
        pair_copy(held.at[me], 0).start()

    def arrive(event):
        if not DO_COMM:
            return
        _, link, half, travel, pieces, follow = event
        ring_copy(link, half, travel, pieces, travel).wait_recv()
        for k, p in follow:
            ring_copy(k, half, travel, p, moved(travel, k)).start()
        dx, dy, dz = travel
        pair_copy(part(chip_of(travel), core, half, pieces), turn_of[(dx % NX, dy, dz % NZ)]).start()

    def turn(stage):
        for copy in read_left(stage):
            copy.wait()

    def turn_tiles(stage, first, last):
        if not DO_TURN:
            return

        def step(t, _):
            at = pl.multiple_of(t * LANES, LANES)
            for n in range(2):
                for h in range(per):
                    tile = left_v[n, stage, h * LANES:(h + 1) * LANES, pl.ds(at, LANES)]
                    row = pl.multiple_of(stage * width + at, LANES)
                    table[pl.ds(row, LANES), n * per + h, :] = tile.astype(jnp.float32).T
            return 0

        lax.fori_loop(first, last, step, 0, unroll=2)

    def pick_some(first):
        if not DO_PICK:
            return
        base = first * depth
        count = RUN * depth

        def fetch(at):
            return tuple(table[order_ref[base + at + u]] for u in range(UNROLL))

        def put(at, got):
            for u in range(UNROLL):
                picked[pl.ds(pl.multiple_of((at + u) * words, words), words), :] = got[u]

        def step(s, got):
            later = fetch(s * UNROLL)
            put(jnp.maximum(s - 1, 0) * UNROLL, got)
            return later

        blank = (jnp.zeros((words, LANES), jnp.float32),) * UNROLL
        put(count - UNROLL, lax.fori_loop(0, count // UNROLL, step, blank))

        def pack(i, _):
            for w in range(words):
                perm[first + i, :, w * LANES:(w + 1) * LANES] = picked[
                    pl.ds(i * depth * words + w, depth, stride=words), :
                ].astype(jnp.bfloat16)
            return 0

        lax.fori_loop(0, RUN, pack, 0)

    work = []
    for stage in range(STAGES):
        work.append((0.0, functools.partial(turn, stage)))
        for t in range(0, width // LANES, TILES):
            work.append((TILES * TURN_US, functools.partial(turn_tiles, stage, t, t + TILES)))
    for b in range(0, devices, RUN):
        work.append((RUN * PICK_US, functools.partial(pick_some, b)))

    def multiply(which):
        def step(_, carry):
            blocks = [chip_of(t) * 2 + w for t in which for w in range(2)]
            lhs = jnp.concatenate([held[b] for b in blocks], axis=1)
            rhs = jnp.concatenate([perm[b] for b in blocks], axis=0)
            acc[...] += jnp.dot(lhs, rhs, preferred_element_type=jnp.float32)
            return carry

        if DO_COMM:
            pair_copy(held.at[pl.ds(0, len(which))], turn_of[which[0]]).wait_recv()
        if DO_MM:
            lax.fori_loop(0, 1, step, 0)

    begin()
    now = 0.0
    todo = list(events)
    for first in range(0, chips, batch):
        which = near[first:first + batch]
        ready = max([e[0] for t in which for e in needs.get(t, [])])
        work.append((MULTIPLY_US, functools.partial(multiply, which), ready + PAIR_US))
    for cost, item, *ready in work:
        now = max([now, *ready])
        while todo and todo[0][0] + SLACK_US <= now:
            arrive(todo.pop(0))
        item()
        now += cost
    assert not todo

    total_devices = devices
    mine = me
    low, high = pl.ds(0, cols), pl.ds(cols, cols)
    scale = scale_ref[...]
    real = (acc[low, 0:rows] - acc[high, rows:2 * rows]) * scale
    imag = (acc[low, rows:2 * rows] + acc[high, 0:rows]) * scale
    squares = jnp.sum(real * real + imag * imag, axis=0, keepdims=True)
    sums[mine] = sum(squares[:, h * LANES:(h + 1) * LANES] for h in range(per))
    out_r[...] = real.T

    def sum_copy(o, which):
        to = lax.rem(mine + o, total_devices)
        return pltpu.make_async_remote_copy(
            src_ref=sums.at[which], dst_ref=sums.at[which],
            send_sem=sum_send, recv_sem=sum_recv,
            device_id={"blk": to}, device_id_type=MESH,
        )

    if DO_COMM:
        for o in range(1, total_devices):
            sum_copy(o, mine).start()
    out_i[...] = imag.T
    if DO_COMM:
        sent = held.at[pl.ds(0, chips - 1)]
        pltpu.make_async_remote_copy(
            src_ref=sent, dst_ref=sent, send_sem=ring_send, recv_sem=sum_recv,
            device_id={"blk": partner}, device_id_type=MESH,
        ).wait_send()
        pair_copy(held.at[pl.ds(0, chips)], 0).wait_send()
        others = sums.at[pl.ds(0, total_devices - 1)]
        exchange = pltpu.make_async_remote_copy(
            src_ref=others, dst_ref=others, send_sem=sum_send, recv_sem=sum_recv,
            device_id={"blk": partner}, device_id_type=MESH,
        )
        exchange.wait_recv()
    total_ref[...] = jnp.sum(jnp.sum(sums[...], axis=0), axis=1, keepdims=True)
    if DO_COMM:
        exchange.wait_send()


def body(devices, groups, left_real, left_imag, right_real, right_imag, row_scale, bond_order):
    rows, bond = left_real.shape
    depth, cols = right_real.shape
    messages = len(plan()[1])
    vmem = pl.BlockSpec(memory_space=pltpu.VMEM)
    far = pl.BlockSpec(memory_space=pl.ANY)
    words = 2 * rows // LANES
    out = jax.ShapeDtypeStruct((rows, cols), jnp.float32)
    real, imag, total = pl.pallas_call(
        functools.partial(kernel, devices),
        out_shape=(out, out, jax.ShapeDtypeStruct((1, 1), jnp.float32)),
        in_specs=[far, far, vmem, vmem, vmem, pl.BlockSpec(memory_space=pltpu.SMEM)],
        out_specs=(vmem, vmem, vmem),
        scratch_shapes=[
            pltpu.VMEM((2, STAGES, rows, bond // STAGES), jnp.bfloat16),
            pltpu.VMEM((bond, words, LANES), jnp.float32),
            pltpu.VMEM((RUN * depth * words, LANES), jnp.float32),
            pltpu.VMEM((devices, depth, 2 * rows), jnp.bfloat16),
            pltpu.VMEM((devices, 2 * cols, depth), jnp.bfloat16),
            pltpu.VMEM((2 * cols, 2 * rows), jnp.float32),
            pltpu.SemaphoreType.DMA((2, STAGES)),
            pltpu.SemaphoreType.DMA,
            pltpu.SemaphoreType.DMA((messages,)),
            pltpu.SemaphoreType.DMA,
            pltpu.SemaphoreType.DMA((8,)),
            pltpu.VMEM((devices, 1, LANES), jnp.float32),
            pltpu.SemaphoreType.DMA,
            pltpu.SemaphoreType.DMA,
        ],
        compiler_params=pltpu.CompilerParams(
            collective_id=0, has_side_effects=True, vmem_limit_bytes=60 * 1024 * 1024
        ),
    )(left_real, left_imag, right_real, right_imag, row_scale.reshape(1, rows), bond_order)
    whole = total
    for o in range(1, groups):
        ring = [(g, (g + o) % groups) for g in range(groups)]
        whole = whole + lax.ppermute(total, "grp", ring)
    factor = 1.0 / jnp.sqrt(whole / jnp.float32(rows * cols * devices * groups))
    return real * factor, imag * factor


def solution(mesh):
    in_specs = (P("blk", None), P("blk", None), P("blk", "grp"), P("blk", "grp"), P("blk"), P())
    out_specs = (P("blk", "grp"), P("blk", "grp"))
    return jax.shard_map(
        functools.partial(body, mesh.shape["blk"], mesh.shape["grp"]),
        mesh=mesh, in_specs=in_specs, out_specs=out_specs, check_vma=False,
    )
```

```python
import functools
import heapq

import jax
import jax.numpy as jnp
from jax import lax
from jax.experimental import pallas as pl
from jax.experimental.pallas import tpu as pltpu
from jax.sharding import PartitionSpec as P

MESH = pl.DeviceIdType.MESH
LANES = 128
HALF = 2
STAGES = 8
UNROLL = 16
TILES = 8
RUN = 8
NX, NY, NZ = 4, 2, 4
DO_COMM, DO_TURN, DO_PICK, DO_MM = True, True, True, True
HOP_US, WIRE_US = 2.4, 0.7
START_US = 2.0
SLACK_US = 0.2
TURN_US, PICK_US = 0.08, 0.18
MULTIPLY_US, PAIR_US = 0.7, 1.2

XP, XM, ZP, ZM, YY = range(5)


def plan():
    events = []
    free = [0.0] * 5
    queue = []
    count = 0

    def send(now, link, half, travel, pieces):
        nonlocal count
        start = max(now, free[link])
        free[link] = start + WIRE_US * len(pieces)
        count += 1
        heapq.heappush(queue, (free[link] + HOP_US, count, link, half, travel, pieces))

    def moved(travel, link):
        dx, dy, dz = travel
        return {
            XP: (dx + 1, dy, dz), XM: (dx - 1, dy, dz), YY: (dx, 1, dz),
            ZP: (dx, dy, dz + 1), ZM: (dx, dy, dz - 1),
        }[link]

    rings = {0: ((XP, XM), (ZP, ZM)), 1: ((ZP, ZM), (XP, XM))}

    def onward(link, half, travel, pieces):
        first, second = rings[half]
        out = []
        stage = 0 if link in first else 1 if link == YY else 2 if link in second else -1
        ring = first if stage == 0 else second if stage == 2 else None
        if ring is not None:
            hops = abs(travel[0] if ring[0] == XP else travel[2])
            if hops == 1:
                mine = tuple(p for p in pieces if p == ring.index(link))
                if mine:
                    out.append((link, mine))
        if stage == -1:
            out += [(k, pieces) for k in first]
        if stage <= 0:
            out.append((YY, pieces))
        if stage <= 1:
            out += [(k, pieces) for k in second]
        return out

    own = [[], []]
    for half in (0, 1):
        own[half] = onward(None, half, (0, 0, 0), (0, 1))
    starts = []
    for pair in zip(*own):
        for half, (link, pieces) in enumerate(pair):
            starts.append((half, link, pieces))
    for half, link, pieces in starts:
        send(0.0, link, half, moved((0, 0, 0), link), pieces)
    while queue:
        now, _, link, half, travel, pieces = heapq.heappop(queue)
        follow = onward(link, half, travel, pieces)
        events.append((now, link, half, travel, pieces, follow))
        for k, p in follow:
            send(now, k, half, moved(travel, k), p)
    return starts, events, moved


def kernel(
    devices,
    lr_hbm, li_hbm, rr_ref, ri_ref, scale_ref, order_ref,
    out_r, out_i, total_ref,
    left_v, table, picked, perm, held, acc,
    left_sem, ring_send, ring_recv, pair_send, pair_recv,
    sums, sum_send, sum_recv,
):
    rows, bond = lr_hbm.shape
    depth, cols = rr_ref.shape
    chips = devices // 2
    per = rows // LANES
    words = 2 * per
    width = bond // STAGES
    piece = 2 * cols // (2 * HALF)

    me = lax.axis_index("blk")
    chip, core = me // 2, lax.rem(me, 2)
    other = 1 - core
    z = lax.rem(chip, NZ)
    y = lax.rem(chip // NZ, NY)
    x = chip // (NZ * NY)
    wrap_x = [lax.rem(x + NX - d, NX) for d in range(NX)]
    wrap_z = [lax.rem(z + NZ - d, NZ) for d in range(NZ)]
    flip_y = [y, 1 - y]

    def chip_of(travel):
        dx, dy, dz = travel
        return (wrap_x[dx % NX] * NY + flip_y[dy]) * NZ + wrap_z[dz % NZ]

    ahead = {
        XP: chip_of((-1, 0, 0)) * 2 + core, XM: chip_of((1, 0, 0)) * 2 + core,
        ZP: chip_of((0, 0, -1)) * 2 + core, ZM: chip_of((0, 0, 1)) * 2 + core,
        YY: chip_of((0, 1, 0)) * 2 + core,
    }
    partner = chip * 2 + other

    def read_left(stage):
        return [
            pltpu.make_async_copy(
                src.at[:, pl.ds(stage * width, width)],
                left_v.at[n, stage],
                left_sem.at[n, stage],
            )
            for n, src in enumerate((lr_hbm, li_hbm))
        ]

    for stage in range(STAGES):
        for copy in read_left(stage):
            copy.start()

    barrier = pltpu.get_barrier_semaphore()
    for target in (*ahead.values(), partner):
        pl.semaphore_signal(barrier, inc=1, device_id={"blk": target}, device_id_type=MESH)

    for n, ref in enumerate((rr_ref, ri_ref)):
        held[me, n * cols:(n + 1) * cols, :] = (
            ref[...].astype(jnp.float32).T.astype(jnp.bfloat16)
        )
    acc[...] = jnp.zeros_like(acc)
    pl.semaphore_wait(barrier, len(ahead) + 1)

    starts, events, moved = plan()
    slots = {}
    for i, (_, link, half, travel, pieces, _) in enumerate(events):
        slots[(link, half, travel, pieces)] = i

    def part(where, which, half, pieces):
        first = (half * HALF + pieces[0]) * piece
        return held.at[where * 2 + which, pl.ds(first, piece * len(pieces)), :]

    def ring_copy(link, half, travel, pieces, after):
        ref = part(chip_of(travel), core, half, pieces)
        return pltpu.make_async_remote_copy(
            src_ref=ref, dst_ref=ref,
            send_sem=ring_send,
            recv_sem=ring_recv.at[slots[(link, half, after, pieces)]],
            device_id={"blk": ahead[link]}, device_id_type=MESH,
        )

    batch = 4
    needs = {}
    for event in events:
        dx, dy, dz = event[3]
        needs.setdefault((dx % NX, dy, dz % NZ), []).append(event)
    near = sorted(needs, key=lambda k: max(e[0] for e in needs[k]))
    near = [(0, 0, 0), *near]
    turn_of = {t: i // batch for i, t in enumerate(near)}

    def pair_copy(ref, slot):
        return pltpu.make_async_remote_copy(
            src_ref=ref, dst_ref=ref, send_sem=pair_send, recv_sem=pair_recv.at[slot],
            device_id={"blk": partner}, device_id_type=MESH,
        )

    def begin():
        if not DO_COMM:
            return
        here = (0, 0, 0)
        for half, link, pieces in starts:
            ring_copy(link, half, here, pieces, moved(here, link)).start()
        pair_copy(held.at[me], 0).start()

    def arrive(event):
        if not DO_COMM:
            return
        _, link, half, travel, pieces, follow = event
        ring_copy(link, half, travel, pieces, travel).wait_recv()
        for k, p in follow:
            ring_copy(k, half, travel, p, moved(travel, k)).start()
        dx, dy, dz = travel
        pair_copy(part(chip_of(travel), core, half, pieces), turn_of[(dx % NX, dy, dz % NZ)]).start()

    def turn(stage):
        for copy in read_left(stage):
            copy.wait()

    flat = table.reshape(bond * words, LANES)

    def turn_tiles(stage, first, last):
        if not DO_TURN:
            return

        def step(t, _):
            at = pl.multiple_of(t * LANES, LANES)
            for n in range(2):
                for h in range(per):
                    tile = left_v[n, stage, h * LANES:(h + 1) * LANES, pl.ds(at, LANES)]
                    row = pl.multiple_of((stage * width + at) * words, LANES) + n * per + h
                    flat[pl.ds(row, LANES, stride=words), :] = tile.astype(jnp.float32).T
            return 0

        lax.fori_loop(first, last, step, 0, unroll=2)

    def pick_some(first):
        if not DO_PICK:
            return
        base = first * depth
        count = RUN * depth

        def fetch(at):
            return tuple(table[order_ref[base + at + u]] for u in range(UNROLL))

        def put(at, got):
            for u in range(UNROLL):
                picked[pl.ds(pl.multiple_of((at + u) * words, words), words), :] = got[u]

        def step(s, got):
            later = fetch(s * UNROLL)
            put(jnp.maximum(s - 1, 0) * UNROLL, got)
            return later

        blank = (jnp.zeros((words, LANES), jnp.float32),) * UNROLL
        put(count - UNROLL, lax.fori_loop(0, count // UNROLL, step, blank))

        def pack(i, _):
            for w in range(words):
                perm[first + i, :, w * LANES:(w + 1) * LANES] = picked[
                    pl.ds(i * depth * words + w, depth, stride=words), :
                ].astype(jnp.bfloat16)
            return 0

        lax.fori_loop(0, RUN, pack, 0)

    work = []
    for stage in range(STAGES):
        work.append((0.0, functools.partial(turn, stage)))
        for t in range(0, width // LANES, TILES):
            work.append((TILES * TURN_US, functools.partial(turn_tiles, stage, t, t + TILES)))
    for b in range(0, devices, RUN):
        work.append((RUN * PICK_US, functools.partial(pick_some, b)))

    def multiply(which):
        def step(_, carry):
            blocks = [chip_of(t) * 2 + w for t in which for w in range(2)]
            lhs = jnp.concatenate([held[b] for b in blocks], axis=1)
            rhs = jnp.concatenate([perm[b] for b in blocks], axis=0)
            acc[...] += jnp.dot(lhs, rhs, preferred_element_type=jnp.float32)
            return carry

        if DO_COMM:
            pair_copy(held.at[pl.ds(0, len(which))], turn_of[which[0]]).wait_recv()
        if DO_MM:
            lax.fori_loop(0, 1, step, 0)

    begin()
    now = 0.0
    todo = list(events)
    for first in range(0, chips, batch):
        which = near[first:first + batch]
        ready = max([e[0] for t in which for e in needs.get(t, [])])
        work.append((MULTIPLY_US, functools.partial(multiply, which), ready + PAIR_US))
    for cost, item, *ready in work:
        now = max([now, *ready])
        while todo and todo[0][0] + SLACK_US <= now:
            arrive(todo.pop(0))
        item()
        now += cost
    assert not todo

    total_devices = devices
    mine = me
    low, high = pl.ds(0, cols), pl.ds(cols, cols)
    scale = scale_ref[...]
    real = (acc[low, 0:rows] - acc[high, rows:2 * rows]) * scale
    imag = (acc[low, rows:2 * rows] + acc[high, 0:rows]) * scale
    squares = jnp.sum(real * real + imag * imag, axis=0, keepdims=True)
    sums[mine] = sum(squares[:, h * LANES:(h + 1) * LANES] for h in range(per))
    out_r[...] = real.T

    def sum_copy(o, which):
        to = lax.rem(mine + o, total_devices)
        return pltpu.make_async_remote_copy(
            src_ref=sums.at[which], dst_ref=sums.at[which],
            send_sem=sum_send, recv_sem=sum_recv,
            device_id={"blk": to}, device_id_type=MESH,
        )

    if DO_COMM:
        for o in range(1, total_devices):
            sum_copy(o, mine).start()
    out_i[...] = imag.T
    if DO_COMM:
        sent = held.at[pl.ds(0, chips - 1)]
        pltpu.make_async_remote_copy(
            src_ref=sent, dst_ref=sent, send_sem=ring_send, recv_sem=sum_recv,
            device_id={"blk": partner}, device_id_type=MESH,
        ).wait_send()
        pair_copy(held.at[pl.ds(0, chips)], 0).wait_send()
        others = sums.at[pl.ds(0, total_devices - 1)]
        exchange = pltpu.make_async_remote_copy(
            src_ref=others, dst_ref=others, send_sem=sum_send, recv_sem=sum_recv,
            device_id={"blk": partner}, device_id_type=MESH,
        )
        exchange.wait_recv()
    total_ref[...] = jnp.sum(jnp.sum(sums[...], axis=0), axis=1, keepdims=True)
    if DO_COMM:
        exchange.wait_send()


def body(devices, groups, left_real, left_imag, right_real, right_imag, row_scale, bond_order):
    rows, bond = left_real.shape
    depth, cols = right_real.shape
    messages = len(plan()[1])
    vmem = pl.BlockSpec(memory_space=pltpu.VMEM)
    far = pl.BlockSpec(memory_space=pl.ANY)
    words = 2 * rows // LANES
    out = jax.ShapeDtypeStruct((rows, cols), jnp.float32)
    real, imag, total = pl.pallas_call(
        functools.partial(kernel, devices),
        out_shape=(out, out, jax.ShapeDtypeStruct((1, 1), jnp.float32)),
        in_specs=[far, far, vmem, vmem, vmem, pl.BlockSpec(memory_space=pltpu.SMEM)],
        out_specs=(vmem, vmem, vmem),
        scratch_shapes=[
            pltpu.VMEM((2, STAGES, rows, bond // STAGES), jnp.bfloat16),
            pltpu.VMEM((bond, words, LANES), jnp.float32),
            pltpu.VMEM((RUN * depth * words, LANES), jnp.float32),
            pltpu.VMEM((devices, depth, 2 * rows), jnp.bfloat16),
            pltpu.VMEM((devices, 2 * cols, depth), jnp.bfloat16),
            pltpu.VMEM((2 * cols, 2 * rows), jnp.float32),
            pltpu.SemaphoreType.DMA((2, STAGES)),
            pltpu.SemaphoreType.DMA,
            pltpu.SemaphoreType.DMA((messages,)),
            pltpu.SemaphoreType.DMA,
            pltpu.SemaphoreType.DMA((8,)),
            pltpu.VMEM((devices, 1, LANES), jnp.float32),
            pltpu.SemaphoreType.DMA,
            pltpu.SemaphoreType.DMA,
        ],
        compiler_params=pltpu.CompilerParams(
            collective_id=0, has_side_effects=True, vmem_limit_bytes=60 * 1024 * 1024
        ),
    )(left_real, left_imag, right_real, right_imag, row_scale.reshape(1, rows), bond_order)
    whole = total
    for o in range(1, groups):
        ring = [(g, (g + o) % groups) for g in range(groups)]
        whole = whole + lax.ppermute(total, "grp", ring)
    factor = 1.0 / jnp.sqrt(whole / jnp.float32(rows * cols * devices * groups))
    return real * factor, imag * factor


def solution(mesh):
    in_specs = (P("blk", None), P("blk", None), P("blk", "grp"), P("blk", "grp"), P("blk"), P())
    out_specs = (P("blk", "grp"), P("blk", "grp"))
    return jax.shard_map(
        functools.partial(body, mesh.shape["blk"], mesh.shape["grp"]),
        mesh=mesh, in_specs=in_specs, out_specs=out_specs, check_vma=False,
    )
```

```python
import functools
import heapq

import jax
import jax.numpy as jnp
from jax import lax
from jax.experimental import pallas as pl
from jax.experimental.pallas import tpu as pltpu
from jax.sharding import PartitionSpec as P

MESH = pl.DeviceIdType.MESH
LANES = 128
HALF = 2
STAGES = 8
UNROLL = 16
TILES = 8
RUN = 8
NX, NY, NZ = 4, 2, 4
DO_COMM, DO_TURN, DO_PICK, DO_MM = True, True, True, True
HOP_US, WIRE_US = 2.4, 0.7
START_US = 2.0
SLACK_US = 0.2
TURN_US, PICK_US = 0.08, 0.18
MULTIPLY_US, PAIR_US = 0.7, 1.2

XP, XM, ZP, ZM, YY = range(5)


def plan():
    events = []
    free = [0.0] * 5
    queue = []
    count = 0

    def send(now, link, half, travel, pieces):
        nonlocal count
        start = max(now, free[link])
        free[link] = start + WIRE_US * len(pieces)
        count += 1
        heapq.heappush(queue, (free[link] + HOP_US, count, link, half, travel, pieces))

    def moved(travel, link):
        dx, dy, dz = travel
        return {
            XP: (dx + 1, dy, dz), XM: (dx - 1, dy, dz), YY: (dx, 1, dz),
            ZP: (dx, dy, dz + 1), ZM: (dx, dy, dz - 1),
        }[link]

    rings = {0: ((XP, XM), (ZP, ZM)), 1: ((ZP, ZM), (XP, XM))}

    def onward(link, half, travel, pieces):
        first, second = rings[half]
        out = []
        stage = 0 if link in first else 1 if link == YY else 2 if link in second else -1
        ring = first if stage == 0 else second if stage == 2 else None
        if ring is not None:
            hops = abs(travel[0] if ring[0] == XP else travel[2])
            if hops == 1:
                mine = tuple(p for p in pieces if p == ring.index(link))
                if mine:
                    out.append((link, mine))
        if stage == -1:
            out += [(k, pieces) for k in first]
        if stage <= 0:
            out.append((YY, pieces))
        if stage <= 1:
            out += [(k, pieces) for k in second]
        return out

    own = [[], []]
    for half in (0, 1):
        own[half] = onward(None, half, (0, 0, 0), (0, 1))
    starts = []
    for pair in zip(*own):
        for half, (link, pieces) in enumerate(pair):
            starts.append((half, link, pieces))
    for half, link, pieces in starts:
        send(0.0, link, half, moved((0, 0, 0), link), pieces)
    while queue:
        now, _, link, half, travel, pieces = heapq.heappop(queue)
        follow = onward(link, half, travel, pieces)
        events.append((now, link, half, travel, pieces, follow))
        for k, p in follow:
            send(now, k, half, moved(travel, k), p)
    return starts, events, moved


def kernel(
    devices, groups,
    lr_hbm, li_hbm, rr_ref, ri_ref, scale_ref, order_ref,
    out_r, out_i, factor_ref,
    left_v, table, picked, perm, held, acc,
    left_sem, ring_send, ring_recv, pair_send, pair_recv,
    sums, sum_send, sum_recv,
):
    rows, bond = lr_hbm.shape
    depth, cols = rr_ref.shape
    chips = devices // 2
    per = rows // LANES
    words = 2 * per
    width = bond // STAGES
    piece = 2 * cols // (2 * HALF)

    me = lax.axis_index("blk")
    my_group = lax.axis_index("grp")
    chip, core = me // 2, lax.rem(me, 2)
    other = 1 - core
    z = lax.rem(chip, NZ)
    y = lax.rem(chip // NZ, NY)
    x = chip // (NZ * NY)
    wrap_x = [lax.rem(x + NX - d, NX) for d in range(NX)]
    wrap_z = [lax.rem(z + NZ - d, NZ) for d in range(NZ)]
    flip_y = [y, 1 - y]

    def chip_of(travel):
        dx, dy, dz = travel
        return (wrap_x[dx % NX] * NY + flip_y[dy]) * NZ + wrap_z[dz % NZ]

    ahead = {
        XP: chip_of((-1, 0, 0)) * 2 + core, XM: chip_of((1, 0, 0)) * 2 + core,
        ZP: chip_of((0, 0, -1)) * 2 + core, ZM: chip_of((0, 0, 1)) * 2 + core,
        YY: chip_of((0, 1, 0)) * 2 + core,
    }
    partner = chip * 2 + other

    def read_left(stage):
        return [
            pltpu.make_async_copy(
                src.at[:, pl.ds(stage * width, width)],
                left_v.at[n, stage],
                left_sem.at[n, stage],
            )
            for n, src in enumerate((lr_hbm, li_hbm))
        ]

    for stage in range(STAGES):
        for copy in read_left(stage):
            copy.start()

    barrier = pltpu.get_barrier_semaphore()
    for target in (*ahead.values(), partner):
        pl.semaphore_signal(barrier, inc=1, device_id={"blk": target}, device_id_type=MESH)
    for o in range(1, groups):
        target = lax.rem(my_group + o, groups)
        pl.semaphore_signal(barrier, inc=1, device_id={"grp": target}, device_id_type=MESH)

    for n, ref in enumerate((rr_ref, ri_ref)):
        held[me, n * cols:(n + 1) * cols, :] = (
            ref[...].astype(jnp.float32).T.astype(jnp.bfloat16)
        )
    acc[...] = jnp.zeros_like(acc)
    pl.semaphore_wait(barrier, len(ahead) + groups)

    starts, events, moved = plan()
    slots = {}
    for i, (_, link, half, travel, pieces, _) in enumerate(events):
        slots[(link, half, travel, pieces)] = i

    def part(where, which, half, pieces):
        first = (half * HALF + pieces[0]) * piece
        return held.at[where * 2 + which, pl.ds(first, piece * len(pieces)), :]

    def ring_copy(link, half, travel, pieces, after):
        ref = part(chip_of(travel), core, half, pieces)
        return pltpu.make_async_remote_copy(
            src_ref=ref, dst_ref=ref,
            send_sem=ring_send,
            recv_sem=ring_recv.at[slots[(link, half, after, pieces)]],
            device_id={"blk": ahead[link]}, device_id_type=MESH,
        )

    batch = 4
    needs = {}
    for event in events:
        dx, dy, dz = event[3]
        needs.setdefault((dx % NX, dy, dz % NZ), []).append(event)
    near = sorted(needs, key=lambda k: max(e[0] for e in needs[k]))
    near = [(0, 0, 0), *near]
    turn_of = {t: i // batch for i, t in enumerate(near)}

    def pair_copy(ref, slot):
        return pltpu.make_async_remote_copy(
            src_ref=ref, dst_ref=ref, send_sem=pair_send, recv_sem=pair_recv.at[slot],
            device_id={"blk": partner}, device_id_type=MESH,
        )

    def begin():
        if not DO_COMM:
            return
        here = (0, 0, 0)
        for half, link, pieces in starts:
            ring_copy(link, half, here, pieces, moved(here, link)).start()
        pair_copy(held.at[me], 0).start()

    def arrive(event):
        if not DO_COMM:
            return
        _, link, half, travel, pieces, follow = event
        ring_copy(link, half, travel, pieces, travel).wait_recv()
        for k, p in follow:
            ring_copy(k, half, travel, p, moved(travel, k)).start()
        dx, dy, dz = travel
        pair_copy(part(chip_of(travel), core, half, pieces), turn_of[(dx % NX, dy, dz % NZ)]).start()

    def turn(stage):
        for copy in read_left(stage):
            copy.wait()

    flat = table.reshape(bond * words, LANES)

    def turn_tiles(stage, first, last):
        if not DO_TURN:
            return

        def step(t, _):
            at = pl.multiple_of(t * LANES, LANES)
            for n in range(2):
                for h in range(per):
                    tile = left_v[n, stage, h * LANES:(h + 1) * LANES, pl.ds(at, LANES)]
                    row = pl.multiple_of((stage * width + at) * words, LANES) + n * per + h
                    flat[pl.ds(row, LANES, stride=words), :] = tile.astype(jnp.float32).T
            return 0

        lax.fori_loop(first, last, step, 0, unroll=2)

    def pick_some(first):
        if not DO_PICK:
            return
        base = first * depth
        count = RUN * depth

        def fetch(at):
            return tuple(table[order_ref[base + at + u]] for u in range(UNROLL))

        def put(at, got):
            for u in range(UNROLL):
                picked[pl.ds(pl.multiple_of((at + u) * words, words), words), :] = got[u]

        def step(s, got):
            later = fetch(s * UNROLL)
            put(jnp.maximum(s - 1, 0) * UNROLL, got)
            return later

        blank = (jnp.zeros((words, LANES), jnp.float32),) * UNROLL
        put(count - UNROLL, lax.fori_loop(0, count // UNROLL, step, blank))

        def pack(i, _):
            for w in range(words):
                perm[first + i, :, w * LANES:(w + 1) * LANES] = picked[
                    pl.ds(i * depth * words + w, depth, stride=words), :
                ].astype(jnp.bfloat16)
            return 0

        lax.fori_loop(0, RUN, pack, 0)

    work = []
    for stage in range(STAGES):
        work.append((0.0, functools.partial(turn, stage)))
        for t in range(0, width // LANES, TILES):
            work.append((TILES * TURN_US, functools.partial(turn_tiles, stage, t, t + TILES)))
    for b in range(0, devices, RUN):
        work.append((RUN * PICK_US, functools.partial(pick_some, b)))

    def multiply(which):
        def step(_, carry):
            blocks = [chip_of(t) * 2 + w for t in which for w in range(2)]
            lhs = jnp.concatenate([held[b] for b in blocks], axis=1)
            rhs = jnp.concatenate([perm[b] for b in blocks], axis=0)
            acc[...] += jnp.dot(lhs, rhs, preferred_element_type=jnp.float32)
            return carry

        if DO_COMM:
            pair_copy(held.at[pl.ds(0, len(which))], turn_of[which[0]]).wait_recv()
        if DO_MM:
            lax.fori_loop(0, 1, step, 0)

    begin()
    now = 0.0
    todo = list(events)
    for first in range(0, chips, batch):
        which = near[first:first + batch]
        ready = max([e[0] for t in which for e in needs.get(t, [])])
        work.append((MULTIPLY_US, functools.partial(multiply, which), ready + PAIR_US))
    for cost, item, *ready in work:
        now = max([now, *ready])
        while todo and todo[0][0] + SLACK_US <= now:
            arrive(todo.pop(0))
        item()
        now += cost
    assert not todo

    total_devices = devices * groups
    mine = my_group * devices + me
    low, high = pl.ds(0, cols), pl.ds(cols, cols)
    scale = scale_ref[...]
    real = (acc[low, 0:rows] - acc[high, rows:2 * rows]) * scale
    imag = (acc[low, rows:2 * rows] + acc[high, 0:rows]) * scale
    squares = jnp.sum(real * real + imag * imag, axis=0, keepdims=True)
    sums[mine] = sum(squares[:, h * LANES:(h + 1) * LANES] for h in range(per))
    out_r[...] = real.T

    def sum_copy(o, which):
        to = lax.rem(mine + o, total_devices)
        return pltpu.make_async_remote_copy(
            src_ref=sums.at[which], dst_ref=sums.at[which],
            send_sem=sum_send, recv_sem=sum_recv,
            device_id={"blk": lax.rem(to, devices), "grp": to // devices},
            device_id_type=MESH,
        )

    if DO_COMM:
        for o in range(1, total_devices):
            sum_copy(o, mine).start()
    out_i[...] = imag.T
    if DO_COMM:
        sent = held.at[pl.ds(0, chips - 1)]
        pltpu.make_async_remote_copy(
            src_ref=sent, dst_ref=sent, send_sem=ring_send, recv_sem=sum_recv,
            device_id={"blk": partner}, device_id_type=MESH,
        ).wait_send()
        pair_copy(held.at[pl.ds(0, chips)], 0).wait_send()
        others = sums.at[pl.ds(0, total_devices - 1)]
        exchange = pltpu.make_async_remote_copy(
            src_ref=others, dst_ref=others, send_sem=sum_send, recv_sem=sum_recv,
            device_id={"blk": partner}, device_id_type=MESH,
        )
        exchange.wait_recv()
    total = jnp.sum(jnp.sum(sums[...], axis=0), axis=1, keepdims=True)
    factor_ref[...] = 1.0 / jnp.sqrt(total / jnp.float32(rows * cols * total_devices))
    if DO_COMM:
        exchange.wait_send()


def body(devices, groups, left_real, left_imag, right_real, right_imag, row_scale, bond_order):
    rows, bond = left_real.shape
    depth, cols = right_real.shape
    messages = len(plan()[1])
    vmem = pl.BlockSpec(memory_space=pltpu.VMEM)
    far = pl.BlockSpec(memory_space=pl.ANY)
    words = 2 * rows // LANES
    out = jax.ShapeDtypeStruct((rows, cols), jnp.float32)
    real, imag, factor = pl.pallas_call(
        functools.partial(kernel, devices, groups),
        out_shape=(out, out, jax.ShapeDtypeStruct((1, 1), jnp.float32)),
        in_specs=[far, far, vmem, vmem, vmem, pl.BlockSpec(memory_space=pltpu.SMEM)],
        out_specs=(vmem, vmem, vmem),
        scratch_shapes=[
            pltpu.VMEM((2, STAGES, rows, bond // STAGES), jnp.bfloat16),
            pltpu.VMEM((bond, words, LANES), jnp.float32),
            pltpu.VMEM((RUN * depth * words, LANES), jnp.float32),
            pltpu.VMEM((devices, depth, 2 * rows), jnp.bfloat16),
            pltpu.VMEM((devices, 2 * cols, depth), jnp.bfloat16),
            pltpu.VMEM((2 * cols, 2 * rows), jnp.float32),
            pltpu.SemaphoreType.DMA((2, STAGES)),
            pltpu.SemaphoreType.DMA,
            pltpu.SemaphoreType.DMA((messages,)),
            pltpu.SemaphoreType.DMA,
            pltpu.SemaphoreType.DMA((8,)),
            pltpu.VMEM((devices * groups, 1, LANES), jnp.float32),
            pltpu.SemaphoreType.DMA,
            pltpu.SemaphoreType.DMA,
        ],
        compiler_params=pltpu.CompilerParams(
            collective_id=0, has_side_effects=True, vmem_limit_bytes=60 * 1024 * 1024
        ),
    )(left_real, left_imag, right_real, right_imag, row_scale.reshape(1, rows), bond_order)
    return real * factor, imag * factor


def solution(mesh):
    in_specs = (P("blk", None), P("blk", None), P("blk", "grp"), P("blk", "grp"), P("blk"), P())
    out_specs = (P("blk", "grp"), P("blk", "grp"))
    return jax.shard_map(
        functools.partial(body, mesh.shape["blk"], mesh.shape["grp"]),
        mesh=mesh, in_specs=in_specs, out_specs=out_specs, check_vma=False,
    )
```
